256 devices in a mesh: dp: 256 (over y, z, x, core).
Axes of the slice: x: 4, y: 4, z: 8, core: 2. Of those that a mesh axis runs over, the one named last changes fastest.
Arguments:
- features: bfloat16 [512, 256, 256], P('dp'), may hold values from -6 to 6
- frame_lens: int32 [512], P('dp'), may hold values from 128 to 256
- labels: int32 [512, 48], P('dp'), may hold values from 1 to 255
- label_lens: int32 [512], P('dp'), may hold values from 1 to 48
- w_up: float32 [262144], P('dp'), may hold values from -0.375 to 0.375
- w_down: float32 [262144], P('dp'), may hold values from -0.1875 to 0.1875
- w_out: float32 [65536], P('dp'), may hold values from -1.125 to 1.125
- first_up: float32 [262144], P('dp'), may hold values from -0.00018 to 0.00018
- first_down: float32 [262144], P('dp'), may hold values from -0.00018 to 0.00018
- first_out: float32 [65536], P('dp'), may hold values from -0.00018 to 0.00018
- second_up: float32 [262144], P('dp'), may hold values from 1e-10 to 1e-08
- second_down: float32 [262144], P('dp'), may hold values from 1e-10 to 1e-08
- second_out: float32 [65536], P('dp'), may hold values from 1e-10 to 1e-08
Outputs:
- new_up: float32 [262144], P('dp')
- new_down: float32 [262144], P('dp')
- new_out: float32 [65536], P('dp')
- new_first_up: float32 [262144], P('dp')
- new_first_down: float32 [262144], P('dp')
- new_first_out: float32 [65536], P('dp')
- new_second_up: float32 [262144], P('dp')
- new_second_down: float32 [262144], P('dp')
- new_second_out: float32 [65536], P('dp')
The draws below stay inside these ranges and needn't reach their ends.
Inputs may be any that keep to these rules, and one draw needn't show every extreme that they name: `labels`: 0 is the blank and is not a label.
All inputs are finite; a program needn't handle non-finite values.
Results may differ from the reference program's by a relative error of at most 0.002.
The reference program's roundings to bfloat16 on the way (of `normalized`, `hidden`, `block_out`, `logit_grad`, `ff_grad` and `act_grad`) count: a program that leaves them out, or rounds other values in their place, can miss the bound.
Values may be sent and summed in bfloat16 or wider, within the bound.
No kernel may reach another device: no remote copies, remote signals or barrier semaphores. Data moves between devices by JAX's collectives and lax.ppermute only.
A program may use at most 64 MiB of HBM per device.

```python
import math
import jax
import jax.numpy as jnp
from jax import lax

D = 256
FF = 1024
VOCAB = 256
UTT = 2
FRAMES = 256
LABELS = 48
UTTERANCES = 512
N_DP = 256


def set_ends(result, rng, smallest, largest):
    longest = result.shape.index(max(result.shape))
    spots = []
    for shift in (0, 1):
        where = [jax.random.randint(jax.random.fold_in(rng, axis), (), 0, length) for axis, length in enumerate(result.shape)]
        where[longest] = (where[longest] + shift) % result.shape[longest]
        spots.append(tuple(where))
    return result.at[spots[0]].set(smallest).at[spots[1]].set(largest)


def shard_levels(rng, shape, cuts, smallest, top_value):
    def one(axis_at, blocks):
        heights = jax.random.uniform(jax.random.fold_in(jax.random.fold_in(rng, 6), axis_at), (blocks,), jnp.float32, smallest / len(cuts), top_value / len(cuts))
        return jnp.repeat(jnp.exp(heights), shape[axis_at] // blocks).reshape((-1,) + (1,) * (len(shape) - axis_at - 1))

    gain = one(*cuts[0])
    for cut in cuts[1:]:
        gain = gain * one(*cut)
    return gain


def gaussian(own_key, dims, deviation, reach, pieces=(), kind=jnp.bfloat16):
    values = jax.random.normal(own_key, dims, jnp.float32) * deviation
    if len(pieces) > 0:
        values = shard_levels(own_key, dims, pieces, -0.22, 0.18) * values
    return jnp.clip(values, min=-reach, max=reach).astype(kind)


def setup_inputs(seed: int = 0) -> dict:
    key_list = jax.random.split(jax.random.key(seed), 14)
    return {
        "features": gaussian(key_list[0], (UTTERANCES, FRAMES, D), 1.0, 6.0, ((0, 256),)),
        "frame_lens": set_ends(jax.random.randint(key_list[1], (UTTERANCES,), FRAMES // 2, FRAMES + 1), jax.random.fold_in(key_list[1], 1), FRAMES // 2, FRAMES).astype(jnp.int32),
        "labels": set_ends(jax.random.randint(key_list[2], (UTTERANCES, LABELS), 1, VOCAB), jax.random.fold_in(key_list[2], 1), 1, VOCAB - 1).astype(jnp.int32),
        "label_lens": set_ends(jax.random.randint(key_list[3], (UTTERANCES,), 1, LABELS + 1), jax.random.fold_in(key_list[3], 1), 1, LABELS).astype(jnp.int32),
        "w_up": gaussian(key_list[4], (D * FF,), D ** -0.5, 0.375, ((0, 256),), jnp.float32),
        "w_down": gaussian(key_list[5], (FF * D,), FF ** -0.5, 0.1875, ((0, 256),), jnp.float32),
        "w_out": gaussian(key_list[6], (D * VOCAB,), (3.0 / D ** 0.5), 1.125, ((0, 256),), jnp.float32),
        "first_up": gaussian(key_list[7], (D * FF,), (3e-5), 0.00018, ((0, 256),), jnp.float32),
        "first_down": gaussian(key_list[8], (FF * D,), (3e-5), 0.00018, ((0, 256),), jnp.float32),
        "first_out": gaussian(key_list[9], (D * VOCAB,), (3e-5), 0.00018, ((0, 256),), jnp.float32),
        "second_up": jnp.clip(jnp.exp(math.log(9.99999993922529e-09) - 4.6051702 * jax.random.uniform(key_list[10], (D * FF,), jnp.float32) ** shard_levels(key_list[10], (D * FF,), ((0, 256),), -0.2, 0.2)), 1.000000013351432e-10, 9.99999993922529e-09),
        "second_down": jnp.clip(jnp.exp(math.log(9.99999993922529e-09) - 4.6051702 * jax.random.uniform(key_list[11], (FF * D,), jnp.float32) ** shard_levels(key_list[11], (FF * D,), ((0, 256),), -0.2, 0.2)), 1.000000013351432e-10, 9.99999993922529e-09),
        "second_out": jnp.clip(jnp.exp(math.log(9.99999993922529e-09) - 4.6051702 * jax.random.uniform(key_list[12], (D * VOCAB,), jnp.float32) ** shard_levels(key_list[12], (D * VOCAB,), ((0, 256),), -0.2, 0.2)), 1.000000013351432e-10, 9.99999993922529e-09),
    }


first_correction = 1.0 - (0.9 ** 10) ** 10
second_correction = 1.0 - (0.999 ** 10) ** 10

def ctc_losses(log_probs, labels, frame_lens, label_lens):
    batch, frames, vocab = log_probs.shape
    label_count = labels.shape[1]
    states = 2 * label_count + 1
    blanks = jnp.zeros_like(labels)
    extended = jnp.concatenate([jnp.stack([blanks, labels], axis=2).reshape(batch, 2 * label_count), blanks[:, :1]], axis=1)
    earlier = jnp.concatenate([jnp.full((batch, 2), -1, jnp.int32), extended[:, :-2]], axis=1)
    may_skip = (extended != 0) & (extended != earlier)
    onehot = (extended[:, :, None] == jnp.arange(vocab, dtype=jnp.int32)[None, None, :]).astype(log_probs.dtype)
    emitted = jnp.einsum('btv,bsv->tbs', log_probs, onehot, precision=lax.Precision.HIGHEST)
    state_ids = jnp.arange(states, dtype=jnp.int32)
    start = jnp.where(state_ids[None, :] < 2, emitted[0], -1e+30)
    frame_ids = jnp.arange(1, frames, dtype=jnp.int32)

    def advance(alpha, inputs):
        emit_row, frame_id = inputs
        lowest = jnp.full((batch, 1), -1e+30, alpha.dtype)
        from_one = jnp.concatenate([lowest, alpha[:, :-1]], axis=1)
        from_two = jnp.concatenate([lowest, lowest, alpha[:, :-2]], axis=1)
        from_two = jnp.where(may_skip, from_two, -1e+30)
        merged = jnp.logaddexp(jnp.logaddexp(alpha, from_one), from_two) + emit_row
        alive = frame_id < frame_lens[:, None]
        return (jnp.where(alive, merged, alpha), None)
    alpha, _ = lax.scan(advance, start, (emitted[1:], frame_ids))
    last_state = 2 * label_lens
    pick_end = lax.optimization_barrier(jnp.sum(jnp.where(state_ids[None, :] == last_state[:, None], alpha, 0.0), axis=1))
    pick_label = lax.optimization_barrier(jnp.sum(jnp.where(state_ids[None, :] == last_state[:, None] - 1, alpha, 0.0), axis=1))
    return -jnp.logaddexp(pick_end, pick_label)

def shard_gradients(features, frame_lens, labels, label_lens, up_mat, down_mat, out_mat, loss_scale):
    batch, frames, width = features.shape
    vocab = out_mat.shape[1]
    flat_in = features.reshape(batch * frames, width).astype(jnp.float32)
    centre = lax.optimization_barrier(jnp.mean(flat_in, axis=1, keepdims=True))
    spread = lax.optimization_barrier(jnp.mean((flat_in - centre) ** 2, axis=1, keepdims=True))
    normalized = ((flat_in - centre) * lax.rsqrt(spread + 1e-05)).astype(jnp.bfloat16)
    activation = jnp.dot(normalized, up_mat, preferred_element_type=jnp.float32)
    hidden = jax.nn.silu(activation).astype(jnp.bfloat16)
    block_out = (flat_in + 0.5 * jnp.dot(hidden, down_mat, preferred_element_type=jnp.float32)).astype(jnp.bfloat16)
    logits = jnp.dot(block_out, out_mat, preferred_element_type=jnp.float32)

    def loss_of(logit_rows):
        log_probs = jax.nn.log_softmax(logit_rows.reshape(batch, frames, vocab), axis=-1)
        return loss_scale * jnp.sum(ctc_losses(log_probs, labels, frame_lens, label_lens))
    loss_value, pullback = jax.vjp(loss_of, logits)
    logit_grad = pullback(jnp.ones((), loss_value.dtype))[0].astype(jnp.bfloat16)
    grad_out = jnp.dot(block_out.T, logit_grad, preferred_element_type=jnp.float32)
    ff_grad = (0.5 * jnp.dot(logit_grad, out_mat.T, preferred_element_type=jnp.float32)).astype(jnp.bfloat16)
    grad_down = jnp.dot(hidden.T, ff_grad, preferred_element_type=jnp.float32)
    sigmoid = jax.nn.sigmoid(activation)
    slope = sigmoid * (1.0 + activation * (1.0 - sigmoid))
    act_grad = (jnp.dot(ff_grad, down_mat.T, preferred_element_type=jnp.float32) * slope).astype(jnp.bfloat16)
    grad_up = jnp.dot(normalized.T, act_grad, preferred_element_type=jnp.float32)
    return (grad_up, grad_down, grad_out)

def adam_update(weight, first, second, grad, clip):
    scaled = clip * grad
    new_first = 0.9 * first + 0.1 * scaled
    new_second = 0.999 * second + 0.001 * scaled * scaled
    ratio = new_first / first_correction / (jnp.sqrt(new_second / second_correction) + 1e-08)
    return (weight - 0.001 * ratio, new_first, new_second)

def reference(features, frame_lens, labels, label_lens, w_up, w_down, w_out, first_up, first_down, first_out, second_up, second_down, second_out):
    up_mat = w_up.astype(jnp.bfloat16).reshape(D, FF)
    down_mat = w_down.astype(jnp.bfloat16).reshape(FF, D)
    out_mat = w_out.astype(jnp.bfloat16).reshape(D, VOCAB)
    loss_scale = 1.0 / (UTT * N_DP)
    shards = (features.reshape(N_DP, UTT, FRAMES, D), frame_lens.reshape(N_DP, UTT), labels.reshape(N_DP, UTT, LABELS), label_lens.reshape(N_DP, UTT))

    def accumulate(carry, item):
        terms = shard_gradients(item[0], item[1], item[2], item[3], up_mat, down_mat, out_mat, loss_scale)
        return ((carry[0] + terms[0], carry[1] + terms[1], carry[2] + terms[2]), None)
    start = (jnp.zeros((D, FF), jnp.float32), jnp.zeros((FF, D), jnp.float32), jnp.zeros((D, VOCAB), jnp.float32))
    sums, _ = lax.scan(accumulate, start, shards)
    grad_up = sums[0].reshape(-1)
    grad_down = sums[1].reshape(-1)
    grad_out = sums[2].reshape(-1)
    total = jnp.sum(grad_up * grad_up) + jnp.sum(grad_down * grad_down) + jnp.sum(grad_out * grad_out)
    clip = 1.0 / jnp.maximum(jnp.sqrt(total), 1.0)
    new_up, new_first_up, new_second_up = adam_update(w_up, first_up, second_up, grad_up, clip)
    new_down, new_first_down, new_second_down = adam_update(w_down, first_down, second_down, grad_down, clip)
    new_out, new_first_out, new_second_out = adam_update(w_out, first_out, second_out, grad_out, clip)
    return (new_up, new_down, new_out, new_first_up, new_first_down, new_first_out, new_second_up, new_second_down, new_second_out)
```

```python
import functools
import math

import jax
import jax.numpy as jnp
from jax import lax
from jax.experimental import pallas as pl
from jax.experimental.pallas import tpu as pltpu
from jax.sharding import Mesh
from jax.sharding import PartitionSpec as P

D = 256
FF = 1024
VOCAB = 256
UTT = 2
FRAMES = 256
LABELS = 48
STATES = 2 * LABELS + 1
LANES = 128
SPAN = 8
BLOCKS = FRAMES // SPAN
BANDS = 2 * SPAN + 1
ROWS = UTT * BLOCKS
SHARE = 2304
LOG2E = math.log2(math.e)
negative = -1e30
first_correction = 1.0 - (0.9**10) ** 10
second_correction = 1.0 - (0.999**10) ** 10
f32 = jnp.float32
bf16 = jnp.bfloat16


def log_sum(terms):
    largest = functools.reduce(jnp.maximum, terms)
    parts = [jnp.exp2(term - largest) for term in terms]
    while len(parts) > 1:
        parts = [sum(parts[i : i + 2]) for i in range(0, len(parts), 2)]
    return largest + jnp.log(parts[0]) * LOG2E


def back(value, amount):
    return value if amount == 0 else pltpu.roll(value, LANES - amount, 1)


def ahead(value, amount):
    return value if amount == 0 else pltpu.roll(value, amount, 1)


def dot_nn(a, b):
    return lax.dot_general(a, b, (((1,), (0,)), ((), ())), preferred_element_type=f32)


def dot_nt(a, b):
    return lax.dot_general(a, b, (((1,), (1,)), ((), ())), preferred_element_type=f32)


def dot_tn(a, b):
    return lax.dot_general(a, b, (((0,), (0,)), ((), ())), preferred_element_type=f32)


def ctc_occupancy(lens, onehot_ref, skip_ref, logit_ref, emit_ref, skips, table, starts, ends, alphas, occ_ref):
    lane = lax.broadcasted_iota(jnp.int32, (1, LANES), 1)
    for u in range(UTT):
        for d in range(BANDS):
            skips[u, d] = back(jnp.broadcast_to(skip_ref[u : u + 1, :], (8, LANES)), d)

    for u in range(UTT):
        value = logit_ref[pl.ds(u * FRAMES, FRAMES), :]
        high = value.astype(bf16)
        rest = value - high.astype(f32)
        middle = rest.astype(bf16)
        low = (rest - middle.astype(f32)).astype(bf16)
        onehot = onehot_ref[u]
        picked = dot_nt(high, onehot) + (dot_nt(middle, onehot) + dot_nt(low, onehot))
        picked = jnp.where(lane < STATES, picked, negative)
        top = jnp.max(picked, axis=1, keepdims=True)
        emit_ref[u] = jnp.where(lane < STATES, (picked - top) * LOG2E, negative)

    def build(group, carry):
        u = group // (BLOCKS // 8)
        first_block = (group % (BLOCKS // 8)) * 8
        frames = lens[u]
        begin = (first_block + lax.broadcasted_iota(jnp.int32, (8, LANES), 0)) * SPAN
        band = [None] * BANDS
        for j in range(SPAN):
            emit = emit_ref[u, pl.ds(first_block * SPAN + j, 8, stride=SPAN), :]
            live = begin + j < frames
            for d in range(2 * j + 2, -1, -1):
                here = back(emit, d)
                if j == 0:
                    new = (here, here, here + skips[u, 2])[d]
                    old = 0.0 if d == 0 else negative
                else:
                    terms = []
                    if d <= 2 * j:
                        terms.append(band[d])
                    if 0 <= d - 1 <= 2 * j:
                        terms.append(band[d - 1])
                    if 0 <= d - 2 <= 2 * j:
                        terms.append(band[d - 2] + skips[u, d])
                    new = (log_sum(terms) if len(terms) > 1 else terms[0]) + here
                    old = negative if band[d] is None else band[d]
                band[d] = jnp.where(live, new, old)
        for d in range(BANDS):
            table[d, pl.ds(group * 8, 8), :] = band[d]
        return carry

    lax.fori_loop(0, ROWS // 8, build, 0)

    row = lax.broadcasted_iota(jnp.int32, (UTT, LANES), 0)
    state = lax.broadcasted_iota(jnp.int32, (UTT, LANES), 1)
    last = 2 * jnp.where(row == 0, lens[2], lens[3])
    alpha = jnp.where(state == 0, 0.0, negative).astype(f32)
    beta = jnp.where((state == last) | (state == last - 1), 0.0, negative).astype(f32)

    def cross(i, carry):
        alpha, beta = carry
        k = BLOCKS - 1 - i
        starts[pl.ds(i, UTT, stride=BLOCKS), :] = alpha
        ends[pl.ds(k, UTT, stride=BLOCKS), :] = beta
        moved = [ahead(table[d, pl.ds(i, UTT, stride=BLOCKS), :] + alpha, d) for d in range(BANDS)]
        returned = [table[d, pl.ds(k, UTT, stride=BLOCKS), :] + back(beta, d) for d in range(BANDS)]
        return log_sum(moved), log_sum(returned)

    lax.fori_loop(0, BLOCKS, cross, (alpha, beta))

    for u in range(UTT):
        rows = pl.ds(u * BLOCKS, BLOCKS)
        frames = lens[u]
        begin = lax.broadcasted_iota(jnp.int32, (BLOCKS, LANES), 0) * SPAN
        skip = skip_ref[u : u + 1, :]
        skip_later = skips[u, 2, 0:1, :]
        now = starts[rows, :]
        for j in range(SPAN):
            emit = emit_ref[u, pl.ds(j, BLOCKS, stride=SPAN), :]
            new = log_sum([now, ahead(now, 1), ahead(now, 2) + skip]) + emit
            now = jnp.where(begin + j < frames, new, now)
            alphas[j] = now
        now = ends[rows, :]
        for j in range(SPAN - 1, -1, -1):
            live = begin + j < frames
            both = alphas[j] + now
            weight = jnp.exp2(both - jnp.max(both, axis=1, keepdims=True))
            share = weight / jnp.sum(weight, axis=1, keepdims=True)
            occ_ref[u, pl.ds(j, BLOCKS, stride=SPAN), :] = jnp.where(live, share, 0.0)
            if j > 0:
                emit = emit_ref[u, pl.ds(j, BLOCKS, stride=SPAN), :]
                passed = now + emit
                new = log_sum([passed, back(passed, 1), back(passed, 2) + skip_later])
                now = jnp.where(live, new, now)


def step_kernel(
    lens, x_ref, w_ref, onehot_ref, skip_ref, grad_ref,
    normal_ref, hidden_ref, slope_ref, block_ref, logit_ref,
    emit_ref, skips, table, starts, ends, alphas, occ_ref, lgrad_ref, fgrad_ref, agrad_ref, *, scale,
):
    chunk = 128

    def forward(c, carry):
        rows = pl.ds(pl.multiple_of(c * chunk, chunk), chunk)
        x = x_ref[rows, :].astype(f32)
        centred = x - jnp.mean(x, axis=1, keepdims=True)
        spread = jnp.mean(centred * centred, axis=1, keepdims=True)
        normal = (centred * lax.rsqrt(spread + 1e-05)).astype(bf16)
        normal_ref[rows, :] = normal
        total = jnp.zeros((chunk, D), f32)
        for q in range(4):
            cols = slice(256 * q, 256 * (q + 1))
            act = dot_nn(normal, w_ref[:, cols])
            sig = 1.0 / (1.0 + jnp.exp(-act))
            hid = (act * sig).astype(bf16)
            hidden_ref[rows, cols] = hid
            slope_ref[rows, cols] = sig * (1.0 + act * (1.0 - sig))
            total = total + dot_nn(hid, w_ref[:, FF + 256 * q : FF + 256 * (q + 1)])
        block = (x + 0.5 * total).astype(bf16)
        block_ref[rows, :] = block
        logit_ref[rows, :] = dot_nn(block, w_ref[:, 2 * FF : SHARE])
        return carry

    lax.fori_loop(0, UTT * FRAMES // chunk, forward, 0)

    ctc_occupancy(lens, onehot_ref, skip_ref, logit_ref, emit_ref, skips, table, starts, ends, alphas, occ_ref)

    def backward(c, carry):
        rows = pl.ds(pl.multiple_of(c * chunk, chunk), chunk)
        u = c // (FRAMES // chunk)
        inside = (c % (FRAMES // chunk)) * chunk
        occ = occ_ref[u, pl.ds(pl.multiple_of(inside, chunk), chunk), :]
        high = occ.astype(bf16)
        low = (occ - high.astype(f32)).astype(bf16)
        onehot = onehot_ref[u]
        gamma = dot_nn(high, onehot) + dot_nn(low, onehot)
        value = logit_ref[rows, :]
        raised = jnp.exp(value - jnp.max(value, axis=1, keepdims=True))
        probs = raised / jnp.sum(raised, axis=1, keepdims=True)
        frame = inside + lax.broadcasted_iota(jnp.int32, (chunk, 1), 0)
        lgrad = jnp.where(frame < lens[u], scale * (probs - gamma), 0.0).astype(bf16)
        lgrad_ref[rows, :] = lgrad
        fgrad = (0.5 * dot_nt(lgrad, w_ref[:, 2 * FF : SHARE])).astype(bf16)
        fgrad_ref[rows, :] = fgrad
        for q in range(4):
            cols = slice(256 * q, 256 * (q + 1))
            back_act = dot_nt(fgrad, w_ref[:, FF + 256 * q : FF + 256 * (q + 1)])
            agrad_ref[rows, cols] = (back_act * slope_ref[rows, cols]).astype(bf16)
        return carry

    lax.fori_loop(0, UTT * FRAMES // chunk, backward, 0)

    kind = grad_ref.dtype
    grad_ref[:, 2 * FF : SHARE] = dot_tn(block_ref[...], lgrad_ref[...]).astype(kind)
    for q in range(4):
        cols = slice(256 * q, 256 * (q + 1))
        grad_ref[:, FF + 256 * q : FF + 256 * (q + 1)] = dot_tn(hidden_ref[:, cols], fgrad_ref[...]).astype(kind)
        grad_ref[:, cols] = dot_tn(normal_ref[...], agrad_ref[:, cols]).astype(kind)


def local_gradients(lens, x, weights, onehot, skip, scale):
    vmem = pl.BlockSpec(memory_space=pltpu.VMEM)
    n = UTT * FRAMES
    return pl.pallas_call(
        functools.partial(step_kernel, scale=scale),
        out_shape=jax.ShapeDtypeStruct((D, SHARE), bf16),
        in_specs=[pl.BlockSpec(memory_space=pltpu.SMEM), vmem, vmem, vmem, vmem],
        out_specs=vmem,
        scratch_shapes=[
            pltpu.VMEM((n, D), bf16),
            pltpu.VMEM((n, FF), bf16),
            pltpu.VMEM((n, FF), f32),
            pltpu.VMEM((n, D), bf16),
            pltpu.VMEM((n, VOCAB), f32),
            pltpu.VMEM((UTT, FRAMES, LANES), f32),
            pltpu.VMEM((UTT, BANDS, 8, LANES), f32),
            pltpu.VMEM((BANDS, ROWS, LANES), f32),
            pltpu.VMEM((ROWS, LANES), f32),
            pltpu.VMEM((ROWS, LANES), f32),
            pltpu.VMEM((SPAN, BLOCKS, LANES), f32),
            pltpu.VMEM((UTT, FRAMES, LANES), f32),
            pltpu.VMEM((n, VOCAB), bf16),
            pltpu.VMEM((n, D), bf16),
            pltpu.VMEM((n, FF), bf16),
        ],
        compiler_params=pltpu.CompilerParams(vmem_limit_bytes=40 * 1024 * 1024),
        name="local_gradients",
    )(lens, x, weights, onehot, skip)


def label_tables(labels):
    blanks = jnp.zeros_like(labels)
    extended = jnp.stack([blanks, labels], axis=2).reshape(UTT, 2 * LABELS)
    extended = jnp.pad(extended, ((0, 0), (0, LANES - 2 * LABELS)))
    earlier = jnp.pad(extended[:, :-2], ((0, 0), (2, 0)), constant_values=-1)
    skip = jnp.where((extended != 0) & (extended != earlier), 0.0, negative).astype(f32)
    valid = jnp.arange(LANES, dtype=jnp.int32) < STATES
    onehot = (extended[:, :, None] == jnp.arange(VOCAB, dtype=jnp.int32)[None, None, :]) & valid[None, :, None]
    return onehot.astype(bf16), skip


def sent_to_all(value, axis):
    copies = jnp.broadcast_to(value, (lax.axis_size(axis), *value.shape))
    return lax.all_to_all(copies, axis, split_axis=0, concat_axis=0, tiled=True)


def adam_update(weight, first, second, grad, clip):
    scaled = clip * grad
    new_first = 0.9 * first + 0.1 * scaled
    new_second = 0.999 * second + 0.001 * scaled * scaled
    ratio = new_first / first_correction / (jnp.sqrt(new_second / second_correction) + 1e-08)
    return (weight - 0.001 * ratio, new_first, new_second)


NEAR = ("x", "core")
FAR = ("y", "z")
ALL = ("y", "z", "x", "core")


def per_device(
    features, frame_lens, labels, label_lens, w_up, w_down, w_out,
    first_up, first_down, first_out, second_up, second_down, second_out,
):
    near, far = lax.axis_size(NEAR), lax.axis_size(FAR)
    up_cut = w_up.astype(bf16).reshape(D, 4).T.reshape(-1)
    packed = jnp.concatenate([up_cut, w_down.astype(bf16), w_out.astype(bf16)])
    weights = sent_to_all(packed, ALL).reshape(near * far, SHARE)
    onehot, skip = label_tables(labels)
    lens = jnp.concatenate([frame_lens, label_lens])
    x = features.reshape(UTT * FRAMES, D)
    grads = local_gradients(lens, x, weights, onehot, skip, 1.0 / (UTT * near * far))
    cut = grads.reshape(far, near, SHARE).swapaxes(0, 1)
    part = jnp.sum(lax.all_to_all(cut, NEAR, 0, 0, tiled=True).astype(f32), axis=0)
    share = jnp.sum(lax.all_to_all(part.astype(bf16), FAR, 0, 0, tiled=True).astype(f32), axis=0)
    squares = jnp.broadcast_to(jnp.sum(share * share), (LANES,))
    squares = jnp.sum(sent_to_all(squares, ALL)[:, 0])
    clip = 1.0 / jnp.maximum(jnp.sqrt(squares), 1.0)
    g_up = share[:FF].reshape(4, D).T.reshape(-1)
    g_down = share[FF : 2 * FF]
    g_out = share[2 * FF :]
    up = adam_update(w_up, first_up, second_up, g_up, clip)
    down = adam_update(w_down, first_down, second_down, g_down, clip)
    out = adam_update(w_out, first_out, second_out, g_out, clip)
    return (up[0], down[0], out[0], up[1], down[1], out[1], up[2], down[2], out[2])


def solution(mesh):
    finer = Mesh(mesh.devices.reshape(4, 8, 4, 2), ALL)
    flat = P(ALL)
    return jax.shard_map(
        per_device,
        mesh=finer,
        in_specs=(P(ALL, None, None), flat, P(ALL, None)) + (flat,) * 10,
        out_specs=(flat,) * 9,
        check_vma=False,
    )
```

```python
import functools
import math

import jax
import jax.numpy as jnp
from jax import lax
from jax.experimental import pallas as pl
from jax.experimental.pallas import tpu as pltpu
from jax.sharding import Mesh
from jax.sharding import PartitionSpec as P

D = 256
FF = 1024
VOCAB = 256
UTT = 2
FRAMES = 256
LABELS = 48
STATES = 2 * LABELS + 1
LANES = 128
SPAN = 8
BLOCKS = FRAMES // SPAN
BANDS = 2 * SPAN + 1
ROWS = UTT * BLOCKS
SHARE = 2304
LOG2E = math.log2(math.e)
negative = -1e30
first_correction = 1.0 - (0.9**10) ** 10
second_correction = 1.0 - (0.999**10) ** 10
f32 = jnp.float32
bf16 = jnp.bfloat16


def log_sum(terms):
    largest = functools.reduce(jnp.maximum, terms)
    parts = [jnp.exp2(term - largest) for term in terms]
    while len(parts) > 1:
        parts = [sum(parts[i : i + 2]) for i in range(0, len(parts), 2)]
    return largest + jnp.log(parts[0]) * LOG2E


def back(value, amount):
    return value if amount == 0 else pltpu.roll(value, LANES - amount, 1)


def ahead(value, amount):
    return value if amount == 0 else pltpu.roll(value, amount, 1)


def dot_nn(a, b):
    return lax.dot_general(a, b, (((1,), (0,)), ((), ())), preferred_element_type=f32)


def dot_nt(a, b):
    return lax.dot_general(a, b, (((1,), (1,)), ((), ())), preferred_element_type=f32)


def dot_tn(a, b):
    return lax.dot_general(a, b, (((0,), (0,)), ((), ())), preferred_element_type=f32)


def ctc_occupancy(lens, onehot_ref, skip_ref, logit_ref, emit_ref, skips, table, starts, ends, alphas, occ_ref):
    lane = lax.broadcasted_iota(jnp.int32, (1, LANES), 1)
    for u in range(UTT):
        for d in range(BANDS):
            skips[u, d] = back(jnp.broadcast_to(skip_ref[u : u + 1, :], (8, LANES)), d)

    for u in range(UTT):
        value = logit_ref[pl.ds(u * FRAMES, FRAMES), :]
        high = value.astype(bf16)
        rest = value - high.astype(f32)
        middle = rest.astype(bf16)
        low = (rest - middle.astype(f32)).astype(bf16)
        onehot = onehot_ref[u]
        picked = dot_nt(high, onehot) + (dot_nt(middle, onehot) + dot_nt(low, onehot))
        picked = jnp.where(lane < STATES, picked, negative)
        top = jnp.max(picked, axis=1, keepdims=True)
        emit_ref[u] = jnp.where(lane < STATES, (picked - top) * LOG2E, negative)

    def build(group, carry):
        u = group // (BLOCKS // 8)
        first_block = (group % (BLOCKS // 8)) * 8
        frames = lens[u]
        begin = (first_block + lax.broadcasted_iota(jnp.int32, (8, LANES), 0)) * SPAN
        band = [None] * BANDS
        for j in range(SPAN):
            emit = emit_ref[u, pl.ds(first_block * SPAN + j, 8, stride=SPAN), :]
            live = begin + j < frames
            for d in range(2 * j + 2, -1, -1):
                here = back(emit, d)
                if j == 0:
                    new = (here, here, here + skips[u, 2])[d]
                    old = 0.0 if d == 0 else negative
                else:
                    terms = []
                    if d <= 2 * j:
                        terms.append(band[d])
                    if 0 <= d - 1 <= 2 * j:
                        terms.append(band[d - 1])
                    if 0 <= d - 2 <= 2 * j:
                        terms.append(band[d - 2] + skips[u, d])
                    new = (log_sum(terms) if len(terms) > 1 else terms[0]) + here
                    old = negative if band[d] is None else band[d]
                band[d] = jnp.where(live, new, old)
        for d in range(BANDS):
            table[d, pl.ds(group * 8, 8), :] = band[d]
        return carry

    lax.fori_loop(0, ROWS // 8, build, 0)

    row = lax.broadcasted_iota(jnp.int32, (UTT, LANES), 0)
    state = lax.broadcasted_iota(jnp.int32, (UTT, LANES), 1)
    last = 2 * jnp.where(row == 0, lens[2], lens[3])
    alpha = jnp.where(state == 0, 0.0, negative).astype(f32)
    beta = jnp.where((state == last) | (state == last - 1), 0.0, negative).astype(f32)

    def cross(i, carry):
        alpha, beta = carry
        k = BLOCKS - 1 - i
        starts[pl.ds(i, UTT, stride=BLOCKS), :] = alpha
        ends[pl.ds(k, UTT, stride=BLOCKS), :] = beta
        moved = [ahead(table[d, pl.ds(i, UTT, stride=BLOCKS), :] + alpha, d) for d in range(BANDS)]
        returned = [table[d, pl.ds(k, UTT, stride=BLOCKS), :] + back(beta, d) for d in range(BANDS)]
        return log_sum(moved), log_sum(returned)

    lax.fori_loop(0, BLOCKS, cross, (alpha, beta))

    for u in range(UTT):
        rows = pl.ds(u * BLOCKS, BLOCKS)
        frames = lens[u]
        begin = lax.broadcasted_iota(jnp.int32, (BLOCKS, LANES), 0) * SPAN
        skip = skip_ref[u : u + 1, :]
        skip_later = skips[u, 2, 0:1, :]
        now = starts[rows, :]
        for j in range(SPAN):
            emit = emit_ref[u, pl.ds(j, BLOCKS, stride=SPAN), :]
            new = log_sum([now, ahead(now, 1), ahead(now, 2) + skip]) + emit
            now = jnp.where(begin + j < frames, new, now)
            alphas[j] = now
        now = ends[rows, :]
        for j in range(SPAN - 1, -1, -1):
            live = begin + j < frames
            both = alphas[j] + now
            weight = jnp.exp2(both - jnp.max(both, axis=1, keepdims=True))
            share = weight / jnp.sum(weight, axis=1, keepdims=True)
            occ_ref[u, pl.ds(j, BLOCKS, stride=SPAN), :] = jnp.where(live, share, 0.0)
            if j > 0:
                emit = emit_ref[u, pl.ds(j, BLOCKS, stride=SPAN), :]
                passed = now + emit
                new = log_sum([passed, back(passed, 1), back(passed, 2) + skip_later])
                now = jnp.where(live, new, now)


def order_of(place, shape, dim):
    i = lax.broadcasted_iota(jnp.int32, shape, dim)
    core = (i & 1) ^ place[1]
    x = ((i >> 1) & 3) ^ place[0]
    return core * 128 + x * 32 + (i >> 3)


def step_kernel(
    lens, place, x_ref, b0, b1, b2, b3, b4, b5, b6, b7, onehot_ref, skip_ref, keep_ref, send_ref,
    w_ref, arrived_ref, normal_ref, hidden_ref, slope_ref, block_ref, logit_ref,
    emit_ref, skips, table, starts, ends, alphas, occ_ref, lgrad_ref, fgrad_ref, agrad_ref, *, scale,
):
    chunk = 128
    for k, block in enumerate((b0, b1, b2, b3, b4, b5, b6, b7)):
        arrived_ref[32 * k : 32 * (k + 1), :] = block[...]
    square = (D, D)
    gather = (order_of(place, square, 0) == lax.broadcasted_iota(jnp.int32, square, 1)).astype(f32).astype(bf16)
    scatter = (order_of(place, square, 1) == lax.broadcasted_iota(jnp.int32, square, 0)).astype(f32).astype(bf16)
    for q in range(9):
        cols = slice(256 * q, 256 * (q + 1))
        w_ref[:, cols] = dot_nn(gather, arrived_ref[:, cols]).astype(bf16)

    def forward(c, carry):
        rows = pl.ds(pl.multiple_of(c * chunk, chunk), chunk)
        x = x_ref[rows, :].astype(f32)
        centred = x - jnp.mean(x, axis=1, keepdims=True)
        spread = jnp.mean(centred * centred, axis=1, keepdims=True)
        normal = (centred * lax.rsqrt(spread + 1e-05)).astype(bf16)
        normal_ref[rows, :] = normal
        total = jnp.zeros((chunk, D), f32)
        for q in range(4):
            cols = slice(256 * q, 256 * (q + 1))
            act = dot_nn(normal, w_ref[:, cols])
            sig = 1.0 / (1.0 + jnp.exp(-act))
            hid = (act * sig).astype(bf16)
            hidden_ref[rows, cols] = hid
            slope_ref[rows, cols] = sig * (1.0 + act * (1.0 - sig))
            total = total + dot_nn(hid, w_ref[:, FF + 256 * q : FF + 256 * (q + 1)])
        block = (x + 0.5 * total).astype(bf16)
        block_ref[rows, :] = block
        logit_ref[rows, :] = dot_nn(block, w_ref[:, 2 * FF : SHARE])
        return carry

    lax.fori_loop(0, UTT * FRAMES // chunk, forward, 0)

    ctc_occupancy(lens, onehot_ref, skip_ref, logit_ref, emit_ref, skips, table, starts, ends, alphas, occ_ref)

    def backward(c, carry):
        rows = pl.ds(pl.multiple_of(c * chunk, chunk), chunk)
        u = c // (FRAMES // chunk)
        inside = (c % (FRAMES // chunk)) * chunk
        occ = occ_ref[u, pl.ds(pl.multiple_of(inside, chunk), chunk), :]
        high = occ.astype(bf16)
        low = (occ - high.astype(f32)).astype(bf16)
        onehot = onehot_ref[u]
        gamma = dot_nn(high, onehot) + dot_nn(low, onehot)
        value = logit_ref[rows, :]
        raised = jnp.exp(value - jnp.max(value, axis=1, keepdims=True))
        probs = raised / jnp.sum(raised, axis=1, keepdims=True)
        frame = inside + lax.broadcasted_iota(jnp.int32, (chunk, 1), 0)
        lgrad = jnp.where(frame < lens[u], scale * (probs - gamma), 0.0).astype(bf16)
        lgrad_ref[rows, :] = lgrad
        fgrad = (0.5 * dot_nt(lgrad, w_ref[:, 2 * FF : SHARE])).astype(bf16)
        fgrad_ref[rows, :] = fgrad
        for q in range(4):
            cols = slice(256 * q, 256 * (q + 1))
            back_act = dot_nt(fgrad, w_ref[:, FF + 256 * q : FF + 256 * (q + 1)])
            agrad_ref[rows, cols] = (back_act * slope_ref[rows, cols]).astype(bf16)
        return carry

    lax.fori_loop(0, UTT * FRAMES // chunk, backward, 0)

    def put(cols, value):
        moved = dot_nn(scatter, value.astype(bf16)).astype(bf16)
        keep_ref[:, cols] = moved[:128]
        send_ref[:, cols] = moved[128:]

    put(slice(2 * FF, SHARE), dot_tn(block_ref[...], lgrad_ref[...]))
    for q in range(4):
        cols = slice(256 * q, 256 * (q + 1))
        put(slice(FF + 256 * q, FF + 256 * (q + 1)), dot_tn(hidden_ref[:, cols], fgrad_ref[...]))
        put(cols, dot_tn(normal_ref[...], agrad_ref[:, cols]))


def local_gradients(lens, place, x, blocks, onehot, skip, scale):
    vmem = pl.BlockSpec(memory_space=pltpu.VMEM)
    smem = pl.BlockSpec(memory_space=pltpu.SMEM)
    n = UTT * FRAMES
    return pl.pallas_call(
        functools.partial(step_kernel, scale=scale),
        out_shape=[jax.ShapeDtypeStruct((D // 2, SHARE), bf16)] * 2,
        in_specs=[smem, smem] + [vmem] * 11,
        out_specs=[vmem, vmem],
        scratch_shapes=[
            pltpu.VMEM((D, SHARE), bf16),
            pltpu.VMEM((D, SHARE), bf16),
            pltpu.VMEM((n, D), bf16),
            pltpu.VMEM((n, FF), bf16),
            pltpu.VMEM((n, FF), f32),
            pltpu.VMEM((n, D), bf16),
            pltpu.VMEM((n, VOCAB), f32),
            pltpu.VMEM((UTT, FRAMES, LANES), f32),
            pltpu.VMEM((UTT, BANDS, 8, LANES), f32),
            pltpu.VMEM((BANDS, ROWS, LANES), f32),
            pltpu.VMEM((ROWS, LANES), f32),
            pltpu.VMEM((ROWS, LANES), f32),
            pltpu.VMEM((SPAN, BLOCKS, LANES), f32),
            pltpu.VMEM((UTT, FRAMES, LANES), f32),
            pltpu.VMEM((n, VOCAB), bf16),
            pltpu.VMEM((n, D), bf16),
            pltpu.VMEM((n, FF), bf16),
        ],
        compiler_params=pltpu.CompilerParams(vmem_limit_bytes=32 * 1024 * 1024),
        name="local_gradients",
    )(lens, place, x, *blocks, onehot, skip)


def label_tables(labels):
    blanks = jnp.zeros_like(labels)
    extended = jnp.stack([blanks, labels], axis=2).reshape(UTT, 2 * LABELS)
    extended = jnp.pad(extended, ((0, 0), (0, LANES - 2 * LABELS)))
    earlier = jnp.pad(extended[:, :-2], ((0, 0), (2, 0)), constant_values=-1)
    skip = jnp.where((extended != 0) & (extended != earlier), 0.0, negative).astype(f32)
    valid = jnp.arange(LANES, dtype=jnp.int32) < STATES
    onehot = (extended[:, :, None] == jnp.arange(VOCAB, dtype=jnp.int32)[None, None, :]) & valid[None, :, None]
    return onehot.astype(bf16), skip


def spread(shape):
    lane = lax.broadcasted_iota(jnp.int32, shape, 0)
    column = lax.broadcasted_iota(jnp.int32, shape, 1)
    return (lane == 4 * (column % 32) + column // D).astype(f32)


def own_rows(shape):
    return (lax.broadcasted_iota(jnp.int32, shape, 1) % D) // 32 == lax.broadcasted_iota(jnp.int32, shape, 0)


def pack_kernel(up_ref, down_ref, out_ref, packed_ref):
    cut = dot_nn(up_ref[...].astype(bf16), spread((LANES, FF)).astype(bf16))
    row = jnp.sum(jnp.where(own_rows((8, FF)), cut, 0.0), axis=0, keepdims=True)
    packed_ref[:, :FF] = row
    packed_ref[:, FF : 2 * FF] = down_ref[...].astype(bf16).astype(f32)
    packed_ref[:, 2 * FF :] = out_ref[...].astype(bf16).astype(f32)


def sum_kernel(arrived_ref, share_ref, square_ref):
    share = jnp.sum(arrived_ref[...].astype(f32), axis=0, keepdims=True)
    share_ref[...] = share
    square_ref[...] = jnp.broadcast_to(jnp.sum(share * share, axis=1, keepdims=True), square_ref.shape)


def adam_update(weight, first, second, grad, clip):
    scaled = clip * grad
    new_first = 0.9 * first + 0.1 * scaled
    new_second = 0.999 * second + 0.001 * scaled * scaled
    ratio = new_first / first_correction / (jnp.sqrt(new_second / second_correction) + 1e-08)
    return (weight - 0.001 * ratio, new_first, new_second)


def adam_kernel(square_ref, share_ref, wu, wd, wo, fu, fd, fo, su, sd, so, *outs):
    total = jnp.sum(square_ref[...], axis=0, keepdims=True)[:, :1]
    clip = 1.0 / jnp.maximum(jnp.sqrt(total), 1.0)
    placed = jnp.where(own_rows((8, FF)), jnp.broadcast_to(share_ref[:, :FF], (8, FF)), 0.0)
    high = placed.astype(bf16)
    rest = placed - high.astype(f32)
    middle = rest.astype(bf16)
    low = (rest - middle.astype(f32)).astype(bf16)
    cut = spread((LANES, FF)).astype(bf16)
    g_up = dot_nt(high, cut) + (dot_nt(middle, cut) + dot_nt(low, cut))
    grads = (g_up, share_ref[:, FF : 2 * FF], share_ref[:, 2 * FF :])
    for k, (w, m, v) in enumerate(((wu, fu, su), (wd, fd, sd), (wo, fo, so))):
        new = adam_update(w[...], m[...], v[...], grads[k], clip)
        for kind in range(3):
            outs[3 * kind + k][...] = new[kind]


def small_call(kernel, shapes, name, *args):
    return pl.pallas_call(
        kernel,
        out_shape=[jax.ShapeDtypeStruct(s, f32) for s in shapes],
        in_specs=[pl.BlockSpec(memory_space=pltpu.VMEM)] * len(args),
        out_specs=[pl.BlockSpec(memory_space=pltpu.VMEM)] * len(shapes),
        compiler_params=pltpu.CompilerParams(vmem_limit_bytes=8 * 1024 * 1024),
        name=name,
    )(*args)


FAR = ("y", "z")
ALL = ("y", "z", "x", "core")


def swap_x(value, k):
    return lax.ppermute(value, "x", [(i, i ^ k) for i in range(4)])


def swap_core(value):
    return lax.ppermute(value, "core", [(0, 1), (1, 0)])


def per_device(
    features, frame_lens, labels, label_lens, w_up, w_down, w_out,
    first_up, first_down, first_out, second_up, second_down, second_out,
):
    far = lax.axis_size(FAR)
    devices = lax.axis_size(ALL)
    views = ((8, LANES), (1, FF), (1, D))
    weights = [w.reshape(s) for w, s in zip((w_up, w_down, w_out), views)]
    firsts = [w.reshape(s) for w, s in zip((first_up, first_down, first_out), views)]
    seconds = [w.reshape(s) for w, s in zip((second_up, second_down, second_out), views)]
    packed = small_call(pack_kernel, [(1, SHARE)], "pack", *weights)[0].astype(bf16)
    copies = jnp.broadcast_to(packed.reshape(1, 2, SHARE // 2), (far, 2, SHARE // 2))
    mine = lax.all_to_all(copies, FAR, 0, 0, tiled=True).reshape(far, SHARE)
    same_core = [mine] + [swap_x(mine, k) for k in (1, 2, 3)]
    blocks = same_core + [swap_core(block) for block in same_core]
    onehot, skip = label_tables(labels)
    lens = jnp.concatenate([frame_lens, label_lens])
    place = jnp.stack([lax.axis_index("x"), lax.axis_index("core")]).astype(jnp.int32)
    x = features.reshape(UTT * FRAMES, D)
    keep, send = local_gradients(lens, place, x, blocks, onehot, skip, 1.0 / (UTT * devices))
    part = keep.astype(f32) + swap_core(send).astype(f32)
    parts = [part[32 * k : 32 * (k + 1)] for k in range(4)]
    arrived = [swap_x(parts[k].astype(bf16), k).astype(f32) for k in (1, 2, 3)]
    total = (parts[0] + arrived[0] + (arrived[1] + arrived[2])).astype(bf16)
    summed = lax.all_to_all(total.reshape(far, 2, SHARE // 2), FAR, 0, 0, tiled=True).reshape(far, SHARE)
    share, square = small_call(sum_kernel, [(1, SHARE), (devices, LANES)], "share", summed)
    squares = lax.all_to_all(square, ALL, 0, 0, tiled=True)
    outs = small_call(adam_kernel, list(views) * 3, "adam", squares, share, *weights, *firsts, *seconds)
    return tuple(value.reshape(-1) for value in outs)


def solution(mesh):
    finer = Mesh(mesh.devices.reshape(4, 8, 4, 2), ALL)
    flat = P(ALL)
    return jax.shard_map(
        per_device,
        mesh=finer,
        in_specs=(P(ALL, None, None), flat, P(ALL, None)) + (flat,) * 10,
        out_specs=(flat,) * 9,
        check_vma=False,
    )
```
